512 devices in a mesh: dp: 4 (over y), row: 16 (over x, z_lo), col: 8 (over z_hi, core).
Axes of the slice: x: 4, y: 4, z: 16 (z_hi: 4, z_lo: 4; z = z_hi * 4 + z_lo), core: 2. Of those that a mesh axis runs over, the one named last changes fastest.
Arguments:
- grad_parts: float32 [4, 4, 1024, 10240], P('dp', None, 'row', 'col'), may hold values from -120 to 120, as said below
- gauss_noise: float32 [4096, 10240], P(('dp', 'row'), 'col'), may hold values from -6 to 6
- blt_buffers: float32 [4, 4096, 10240], P(None, ('dp', 'row'), 'col'), may hold values from -4 to 4
- blt_decays: float32 [4], replicated, may hold values from 0.2 to 0.98
- blt_weights: float32 [4], replicated, may hold values from 0.1 to 0.6
- master_weights: float32 [4096, 10240], P(('dp', 'row'), 'col'), may hold values from -4 to 4
- row_stat: float32 [4096], P(('dp', 'row')), may hold values from 0.05 to 0.5
- col_stat: float32 [10240], P('col'), may hold values from 0.05 to 0.5
Outputs:
- direction: float32 [4096, 10240], P(('dp', 'row'), 'col')
- weight_copy: bfloat16 [4096, 10240], P(('dp', 'row'), 'col')
- new_buffers: float32 [4, 4096, 10240], P(None, ('dp', 'row'), 'col')
- new_row_stat: float32 [4096], P(('dp', 'row'))
- new_col_stat: float32 [10240], P('col')
The draws below stay inside these ranges and needn't reach their ends.
Inputs may be any that keep to these rules, and one draw needn't show every extreme that they name: `grad_parts`: finite real values.
All inputs are finite; a program needn't handle non-finite values.
Results may differ from the reference program's by a relative error of at most 0.001.
Values sent between devices are 32-bit elements; how exact they have to be, the bound alone decides.
No kernel may reach another device: no remote copies, remote signals or barrier semaphores. Data moves between devices by JAX's collectives and lax.ppermute only.
A program may use at most 64 MiB of HBM per device.

```python
import math
import jax
import jax.numpy as jnp
from jax import lax

D = 4096
FF = 10240
BUFFERS = 4
N_DP = 4


def draw_grad_parts(key, part):
    first, second, third = jax.random.split(key, 3)
    row_pos = jnp.arange(D, dtype=jnp.float32) / (D - 1)
    col_pos = jnp.arange(FF, dtype=jnp.float32) / (FF - 1)
    row_scale = 0.1 * 5.0 ** row_pos * 10.0 ** jax.random.uniform(first, (D,), jnp.float32)
    col_scale = 0.1 * 3.0 ** col_pos * 10.0 ** jax.random.uniform(second, (FF,), jnp.float32)
    scales = (row_scale[:, None] * col_scale[None, :]).reshape(1, N_DP, D // N_DP, FF)
    entries = jax.random.truncated_normal(third, -5.0, 5.0, (N_DP, N_DP, D // N_DP, FF), jnp.float32)
    return (entries * scales).astype(jnp.float32)


def shard_levels(own_key, dims, cuts, smallest, largest):
    loudness = 1.0
    for position, parts in cuts:
        heights = jax.random.uniform(jax.random.fold_in(jax.random.fold_in(own_key, 6), position), (parts,), jnp.float32, smallest / len(cuts), largest / len(cuts))
        loudness = loudness * jnp.repeat(jnp.exp(heights), dims[position] // parts).reshape((-1,) + (1,) * (len(dims) - 1 - position))
    return loudness


def normal_values(rng, dims, deviation, reach, shards=(), kind=jnp.bfloat16):
    result = deviation * jax.random.normal(rng, dims, jnp.float32)
    if shards:
        result = result * shard_levels(rng, dims, shards, -0.22, 0.18)
    return jnp.clip(result, -reach, reach).astype(kind)


def setup_inputs(seed: int = 0) -> dict:
    seeds = jax.random.split(jax.random.key(seed), 9)
    grad_parts = draw_grad_parts(jax.random.fold_in(seeds[8], 71), 0)
    gauss_noise = normal_values(seeds[1], (D, FF), 1.0, 6.0, ((0, 64), (1, 8)), jnp.float32)
    blt_buffers = normal_values(seeds[2], (BUFFERS, D, FF), 0.5, 4.0, ((1, 64), (2, 8)), jnp.float32)
    blt_decays = jnp.clip(jnp.exp(jax.random.uniform(seeds[3], (BUFFERS,), jnp.float32, math.log(0.2), math.log(0.98))), 0.2, 0.98)
    blt_weights = jnp.clip(jax.random.uniform(seeds[4], (BUFFERS,), jnp.float32, 0.1, 0.6), 0.1, 0.6)
    master_weights = normal_values(seeds[5], (D, FF), 0.5, 4.0, ((0, 64), (1, 8)), jnp.float32)
    row_stat = jnp.clip(jnp.exp(math.log(0.5) - 2.3025851 * jax.random.uniform(seeds[6], (D,), jnp.float32) ** shard_levels(seeds[6], (D,), ((0, 64),), -0.2, 0.2)), 0.05, 0.5)
    col_stat = jnp.clip(jnp.exp(math.log(0.5) - 2.3025851 * jax.random.uniform(seeds[7], (FF,), jnp.float32) ** shard_levels(seeds[7], (FF,), ((0, 8),), -0.2, 0.2)), 0.05, 0.5)
    return {"grad_parts": grad_parts, "gauss_noise": gauss_noise, "blt_buffers": blt_buffers, "blt_decays": blt_decays, "blt_weights": blt_weights, "master_weights": master_weights, "row_stat": row_stat, "col_stat": col_stat}


NOISE_STD = 2.0
DECAY_RATE = 0.85
LEARN_RATE = 0.01
TINY_TERM = 1e-30

def reference(grad_parts, gauss_noise, blt_buffers, blt_decays, blt_weights, master_weights, row_stat, col_stat):
    grad_sum = lax.optimization_barrier(jnp.sum(grad_parts, axis=0)).reshape(D, FF)
    correlated = gauss_noise - lax.optimization_barrier(jnp.sum(blt_buffers * blt_weights[:, None, None], axis=0))
    noisy = grad_sum + NOISE_STD * correlated
    new_buffers = blt_decays[:, None, None] * blt_buffers + correlated[None]
    squares = noisy * noisy
    new_row = DECAY_RATE * row_stat + (1.0 - DECAY_RATE) * (lax.optimization_barrier(jnp.mean(squares, axis=1)) + TINY_TERM)
    new_col = DECAY_RATE * col_stat + (1.0 - DECAY_RATE) * (lax.optimization_barrier(jnp.mean(squares, axis=0)) + TINY_TERM)
    row_mean = jnp.mean(new_row)
    direction = noisy / jnp.sqrt(new_row[:, None] * new_col[None, :] / row_mean)
    weight_copy = (master_weights - LEARN_RATE * direction).astype(jnp.bfloat16)
    return (direction, weight_copy, new_buffers, new_row, new_col)
```

```python
import jax
import jax.numpy as jnp
from jax import lax
from jax.sharding import Mesh
from jax.sharding import PartitionSpec as P


D = 4096
FF = 10240
NOISE_STD = 2.0
DECAY_RATE = 0.85
LEARN_RATE = 0.01
TINY_TERM = 1e-30

ROW = ("x", "zl")
COL = ("zh", "core")
DEPTH = ("zl", "zh", "core")
PLANE = ("dp", "x")


def from_all(shard, axes):
    n = lax.axis_size(axes)
    copies = jnp.broadcast_to(shard[None], (n, *shard.shape))
    return lax.all_to_all(copies, axes, split_axis=0, concat_axis=0, tiled=True)


def per_device(
    grad_parts,
    gauss_noise,
    blt_buffers,
    blt_decays,
    blt_weights,
    master_weights,
    row_stat,
    col_stat,
):
    rows, cols = gauss_noise.shape
    n_col = lax.axis_size(COL)
    arrived = lax.all_to_all(
        grad_parts.reshape(-1, rows, cols), "dp", split_axis=0, concat_axis=0, tiled=True
    )
    correlated = gauss_noise - jnp.sum(blt_buffers * blt_weights[:, None, None], axis=0)
    new_buffers = blt_decays[:, None, None] * blt_buffers + correlated[None]
    arrived, correlated, new_buffers = lax.optimization_barrier((arrived, correlated, new_buffers))
    noisy = arrived.sum(axis=0) + NOISE_STD * correlated
    squares = noisy * noisy
    share = DECAY_RATE / n_col * row_stat + (1.0 - DECAY_RATE) * (
        jnp.sum(squares, axis=1) / FF + TINY_TERM / n_col
    )
    col_part = jnp.sum(squares, axis=0)
    shares = from_all(share, DEPTH)
    col_parts = from_all(col_part, "zl")
    shares = shares.reshape(-1, n_col, rows).sum(axis=1)
    new_row = lax.dynamic_index_in_dim(shares, lax.axis_index("zl"), 0, keepdims=False)
    packed = jnp.concatenate([col_parts.sum(axis=0), shares.sum(axis=0)])
    packs = from_all(packed, PLANE).sum(axis=0)
    new_col = DECAY_RATE * col_stat + (1.0 - DECAY_RATE) * (packs[:cols] / D + TINY_TERM)
    row_mean = jnp.sum(packs[cols:]) / D
    direction = noisy / jnp.sqrt(new_row[:, None] * new_col[None, :] / row_mean)
    weight_copy = (master_weights - LEARN_RATE * direction).astype(jnp.bfloat16)
    return (direction, weight_copy, new_buffers, new_row, new_col)


def solution(mesh):
    finer = Mesh(
        mesh.devices.reshape(mesh.shape["dp"], 4, 4, 4, 2),
        ("dp", "x", "zl", "zh", "core"),
    )
    rows = ("dp", *ROW)
    return jax.shard_map(
        per_device,
        mesh=finer,
        in_specs=(
            P("dp", None, ROW, COL),
            P(rows, COL),
            P(None, rows, COL),
            P(),
            P(),
            P(rows, COL),
            P(rows),
            P(COL),
        ),
        out_specs=(P(rows, COL), P(rows, COL), P(None, rows, COL), P(rows), P(COL)),
        check_vma=False,
    )
```

```python
import jax
import jax.numpy as jnp
from jax import lax
from jax.sharding import Mesh
from jax.sharding import PartitionSpec as P

D = 4096
FF = 10240
NOISE_STD = 2.0
DECAY_RATE = 0.85
LEARN_RATE = 0.01
TINY_TERM = 1e-30

ROW = ("x", "zl")
COL = ("zh", "core")
RUN = ("zl", "core")
PLANE = ("dp", "x")


def sum_of_sent(messages, axes):
    arrived = lax.all_to_all(messages, axes, split_axis=0, concat_axis=0, tiled=True)
    return arrived.sum(axis=0)


def per_device(
    grad_parts,
    gauss_noise,
    blt_buffers,
    blt_decays,
    blt_weights,
    master_weights,
    row_stat,
    col_stat,
):
    rows, cols = gauss_noise.shape
    n_col, n_run, n_plane = (lax.axis_size(axes) for axes in (COL, RUN, PLANE))
    arrived = lax.all_to_all(
        grad_parts.reshape(-1, rows, cols), "dp", split_axis=0, concat_axis=0, tiled=True
    )
    correlated = gauss_noise - jnp.sum(blt_buffers * blt_weights[:, None, None], axis=0)
    new_buffers = blt_decays[:, None, None] * blt_buffers + correlated[None]
    to = jnp.arange(n_run)
    same_cols = (to % 2 == lax.axis_index("core")).astype(jnp.float32)
    same_rows = (to // 2 == lax.axis_index("zl")).astype(jnp.float32)
    takes = jnp.concatenate(
        [
            jnp.broadcast_to(same_cols[:, None], (n_run, cols)),
            jnp.ones((n_run, rows), jnp.float32),
            jnp.broadcast_to(same_rows[:, None], (n_run, rows)),
        ],
        axis=1,
    )
    ones = jnp.broadcast_to(same_cols[0] + same_cols[1], (rows, rows))
    arrived, correlated, new_buffers, takes, row_stat, ones = lax.optimization_barrier(
        (arrived, correlated, new_buffers, takes, row_stat, ones)
    )
    noisy = arrived.sum(axis=0) + NOISE_STD * correlated
    squares = noisy * noisy
    share = DECAY_RATE / n_col * row_stat + (1.0 - DECAY_RATE) * (
        jnp.sum(squares, axis=1) / FF + TINY_TERM / n_col
    )
    sums = jnp.concatenate([jnp.sum(squares, axis=0), share, share])
    sums, col_stat, master_weights, takes = lax.optimization_barrier(
        (sums, col_stat, master_weights, takes)
    )
    run = sum_of_sent(sums[None] * takes, RUN)
    run, own = lax.optimization_barrier((run, run[cols + rows :]))
    plane = sum_of_sent(jnp.broadcast_to(run[None], (n_plane, *run.shape)), PLANE)
    stats = jnp.concatenate([plane[cols : cols + rows], own])
    new_col = DECAY_RATE * col_stat + (1.0 - DECAY_RATE) * (plane[:cols] / D + TINY_TERM)
    stats, new_col = lax.optimization_barrier((stats, new_col))
    stats = lax.psum(stats, "zh")
    shares, new_row = lax.optimization_barrier((stats[:rows], stats[rows:]))
    row_mean = jnp.sum(ones * shares[None, :], axis=1) / D
    direction = noisy / jnp.sqrt((new_row / row_mean)[:, None] * new_col[None, :])
    weight_copy = (master_weights - LEARN_RATE * direction).astype(jnp.bfloat16)
    return (direction, weight_copy, new_buffers, new_row, new_col)


def solution(mesh):
    finer = Mesh(
        mesh.devices.reshape(mesh.shape["dp"], 4, 4, 4, 2),
        ("dp", "x", "zl", "zh", "core"),
    )
    rows = ("dp", *ROW)
    return jax.shard_map(
        per_device,
        mesh=finer,
        in_specs=(
            P("dp", None, ROW, COL),
            P(rows, COL),
            P(None, rows, COL),
            P(),
            P(),
            P(rows, COL),
            P(rows),
            P(COL),
        ),
        out_specs=(P(rows, COL), P(rows, COL), P(None, rows, COL), P(rows), P(COL)),
        check_vma=False,
    )
```

```python
import jax
import jax.numpy as jnp
from jax import lax
from jax.sharding import Mesh
from jax.sharding import PartitionSpec as P


D = 4096
FF = 10240
NOISE_STD = 2.0
DECAY_RATE = 0.85
LEARN_RATE = 0.01
TINY_TERM = 1e-30

ROW = ("x", "zl")
COL = ("zh", "core")
RUN = ("zl", "core")
PLANE = ("dp", "x")


def sum_of_sent(messages, axes):
    arrived = lax.all_to_all(messages, axes, split_axis=0, concat_axis=0, tiled=True)
    return arrived.sum(axis=0)


def sum_over_zh(mine, part_01, part_23, is_01, is_1, is_3):
    def push(values, *pairs):
        return lax.ppermute(values, "zh", pairs)

    n = mine.shape[0]
    again = lax.optimization_barrier(mine)
    a = push(mine, (2, 0))
    b = push(mine, (3, 0))
    c = push(mine, (1, 0), (2, 1))
    d = push(jnp.concatenate([mine, b]), (0, 1), (2, 3))
    e = push(mine + c, (0, 3), (3, 2))
    f = push(again + d[:n], (1, 2))
    is_0, is_2 = is_01 - is_1, 1.0 - is_01 - is_3
    from_01 = part_01 + is_0 * c + is_1 * d[:n] + is_3 * e + f
    from_23 = part_23 + a + b + is_1 * c + d[n:] + is_3 * d[:n] + is_2 * e
    return from_01 + from_23


def per_device(
    grad_parts,
    gauss_noise,
    blt_buffers,
    blt_decays,
    blt_weights,
    master_weights,
    row_stat,
    col_stat,
):
    rows, cols = gauss_noise.shape
    n_col, n_run, n_plane = (lax.axis_size(axes) for axes in (COL, RUN, PLANE))
    arrived = lax.all_to_all(
        grad_parts.reshape(-1, rows, cols), "dp", split_axis=0, concat_axis=0, tiled=True
    )
    correlated = gauss_noise - jnp.sum(blt_buffers * blt_weights[:, None, None], axis=0)
    new_buffers = blt_decays[:, None, None] * blt_buffers + correlated[None]
    to = jnp.arange(n_run)
    same_cols = (to % 2 == lax.axis_index("core")).astype(jnp.float32)
    same_rows = (to // 2 == lax.axis_index("zl")).astype(jnp.float32)
    takes = jnp.concatenate(
        [
            jnp.broadcast_to(same_cols[:, None], (n_run, cols)),
            jnp.ones((n_run, rows), jnp.float32),
            jnp.broadcast_to(same_rows[:, None], (n_run, rows)),
        ],
        axis=1,
    )
    ones = jnp.broadcast_to(same_cols[0] + same_cols[1], (rows, rows))
    zh = lax.axis_index("zh")
    is_01, is_1, is_3 = (
        jnp.broadcast_to(here.astype(jnp.float32), (2 * rows,)) for here in (zh < 2, zh == 1, zh == 3)
    )
    arrived, correlated, new_buffers, takes, row_stat, ones, is_01, is_1, is_3 = lax.optimization_barrier(
        (arrived, correlated, new_buffers, takes, row_stat, ones, is_01, is_1, is_3)
    )
    noisy = arrived.sum(axis=0) + NOISE_STD * correlated
    squares = noisy * noisy
    share = DECAY_RATE / n_col * row_stat + (1.0 - DECAY_RATE) * (
        jnp.sum(squares, axis=1) / FF + TINY_TERM / n_col
    )
    sums = jnp.concatenate([jnp.sum(squares, axis=0), share, share])
    sums, col_stat, master_weights, takes = lax.optimization_barrier(
        (sums, col_stat, master_weights, takes)
    )
    run = sum_of_sent(sums[None] * takes, RUN)
    run, own = lax.optimization_barrier((run, run[cols + rows :]))
    plane = sum_of_sent(jnp.broadcast_to(run[None], (n_plane, *run.shape)), PLANE)
    stats = jnp.concatenate([plane[cols : cols + rows], own])
    new_col = DECAY_RATE * col_stat + (1.0 - DECAY_RATE) * (plane[:cols] / D + TINY_TERM)
    part_01, part_23 = is_01 * stats, (1.0 - is_01) * stats
    stats, new_col, part_01, part_23 = lax.optimization_barrier((stats, new_col, part_01, part_23))
    stats = sum_over_zh(stats, part_01, part_23, is_01, is_1, is_3)
    shares, new_row = lax.optimization_barrier((stats[:rows], stats[rows:]))
    row_mean = jnp.sum(ones * shares[None, :], axis=1) / D
    direction = noisy / jnp.sqrt((new_row / row_mean)[:, None] * new_col[None, :])
    weight_copy = (master_weights - LEARN_RATE * direction).astype(jnp.bfloat16)
    return (direction, weight_copy, new_buffers, new_row, new_col)


def solution(mesh):
    finer = Mesh(
        mesh.devices.reshape(mesh.shape["dp"], 4, 4, 4, 2),
        ("dp", "x", "zl", "zh", "core"),
    )
    rows = ("dp", *ROW)
    return jax.shard_map(
        per_device,
        mesh=finer,
        in_specs=(
            P("dp", None, ROW, COL),
            P(rows, COL),
            P(None, rows, COL),
            P(),
            P(),
            P(rows, COL),
            P(rows),
            P(COL),
        ),
        out_specs=(P(rows, COL), P(rows, COL), P(None, rows, COL), P(rows), P(COL)),
        check_vma=False,
    )
```

```python
import jax
import jax.numpy as jnp
from jax import lax
from jax.sharding import Mesh
from jax.sharding import PartitionSpec as P


D = 4096
FF = 10240
NOISE_STD = 2.0
DECAY_RATE = 0.85
LEARN_RATE = 0.01
TINY_TERM = 1e-30

ROW = ("x", "zl")
COL = ("zh", "core")
RUN = ("zl", "core")
PLANE = ("dp", "x")


def sum_of_sent(messages, axes):
    arrived = lax.all_to_all(messages, axes, split_axis=0, concat_axis=0, tiled=True)
    return arrived.sum(axis=0)


def sum_over_zh(mine, part_01, part_23, is_01, is_1, is_3):
    def push(values, *pairs):
        return lax.ppermute(values, "zh", pairs)

    n = mine.shape[0]
    again = lax.optimization_barrier(mine)
    a = push(mine, (2, 0))
    b = push(mine, (3, 0))
    c = push(mine, (1, 0), (2, 1))
    d = push(jnp.concatenate([mine, b]), (0, 1), (2, 3))
    e = push(mine + c, (0, 3))
    f = push(jnp.concatenate([e, again]), (3, 2))
    is_0 = is_01 - is_1
    from_01 = part_01 + is_0 * c + is_1 * d[:n] + e + f[:n]
    from_23 = part_23 + a + b + is_1 * c + d[n:] + is_3 * d[:n] + f[n:]
    return from_01 + from_23


def per_device(
    grad_parts,
    gauss_noise,
    blt_buffers,
    blt_decays,
    blt_weights,
    master_weights,
    row_stat,
    col_stat,
):
    rows, cols = gauss_noise.shape
    n_col, n_run, n_plane = (lax.axis_size(axes) for axes in (COL, RUN, PLANE))
    arrived = lax.all_to_all(
        grad_parts.reshape(-1, rows, cols), "dp", split_axis=0, concat_axis=0, tiled=True
    )
    correlated = gauss_noise - jnp.sum(blt_buffers * blt_weights[:, None, None], axis=0)
    new_buffers = blt_decays[:, None, None] * blt_buffers + correlated[None]
    to = jnp.arange(n_run)
    same_cols = (to % 2 == lax.axis_index("core")).astype(jnp.float32)
    same_rows = (to // 2 == lax.axis_index("zl")).astype(jnp.float32)
    takes = jnp.concatenate(
        [
            jnp.broadcast_to(same_cols[:, None], (n_run, cols)),
            jnp.ones((n_run, rows), jnp.float32),
            jnp.broadcast_to(same_rows[:, None], (n_run, rows)),
        ],
        axis=1,
    )
    ones = jnp.broadcast_to(same_cols[0] + same_cols[1], (rows, rows))
    zh = lax.axis_index("zh")
    is_01, is_1, is_3 = (
        jnp.broadcast_to(here.astype(jnp.float32), (2 * rows,)) for here in (zh < 2, zh == 1, zh == 3)
    )
    arrived, correlated, new_buffers, takes, row_stat, ones, is_01, is_1, is_3 = lax.optimization_barrier(
        (arrived, correlated, new_buffers, takes, row_stat, ones, is_01, is_1, is_3)
    )
    noisy = arrived.sum(axis=0) + NOISE_STD * correlated
    squares = noisy * noisy
    share = DECAY_RATE / n_col * row_stat + (1.0 - DECAY_RATE) * (
        jnp.sum(squares, axis=1) / FF + TINY_TERM / n_col
    )
    sums = jnp.concatenate([jnp.sum(squares, axis=0), share, share])
    sums, col_stat, master_weights, takes = lax.optimization_barrier(
        (sums, col_stat, master_weights, takes)
    )
    run = sum_of_sent(sums[None] * takes, RUN)
    run, own = lax.optimization_barrier((run, run[cols + rows :]))
    plane = sum_of_sent(jnp.broadcast_to(run[None], (n_plane, *run.shape)), PLANE)
    stats = jnp.concatenate([plane[cols : cols + rows], own])
    new_col = DECAY_RATE * col_stat + (1.0 - DECAY_RATE) * (plane[:cols] / D + TINY_TERM)
    part_01, part_23 = is_01 * stats, (1.0 - is_01) * stats
    stats, new_col, part_01, part_23 = lax.optimization_barrier((stats, new_col, part_01, part_23))
    stats = sum_over_zh(stats, part_01, part_23, is_01, is_1, is_3)
    shares, new_row = lax.optimization_barrier((stats[:rows], stats[rows:]))
    row_mean = jnp.sum(ones * shares[None, :], axis=1) / D
    direction = noisy / jnp.sqrt((new_row / row_mean)[:, None] * new_col[None, :])
    weight_copy = (master_weights - LEARN_RATE * direction).astype(jnp.bfloat16)
    return (direction, weight_copy, new_buffers, new_row, new_col)


def solution(mesh):
    finer = Mesh(
        mesh.devices.reshape(mesh.shape["dp"], 4, 4, 4, 2),
        ("dp", "x", "zl", "zh", "core"),
    )
    rows = ("dp", *ROW)
    return jax.shard_map(
        per_device,
        mesh=finer,
        in_specs=(
            P("dp", None, ROW, COL),
            P(rows, COL),
            P(None, rows, COL),
            P(),
            P(),
            P(rows, COL),
            P(rows),
            P(COL),
        ),
        out_specs=(P(rows, COL), P(rows, COL), P(None, rows, COL), P(rows), P(COL)),
        check_vma=False,
    )
```

```python
import jax
import jax.numpy as jnp
from jax import lax
from jax.sharding import Mesh
from jax.sharding import PartitionSpec as P


D = 4096
FF = 10240
NOISE_STD = 2.0
DECAY_RATE = 0.85
LEARN_RATE = 0.01
TINY_TERM = 1e-30

ROW = ("x", "zl")
COL = ("zh", "core")
RUN = ("zl", "core")
PLANE = ("dp", "x")


def sum_of_sent(messages, axes):
    arrived = lax.all_to_all(messages, axes, split_axis=0, concat_axis=0, tiled=True)
    return arrived.sum(axis=0)


def sum_over_zh(mine, part_01, part_23, is_1, is_3):
    def push(values, *pairs):
        return lax.ppermute(values, "zh", pairs)

    n = mine.shape[0]
    again = lax.optimization_barrier(mine)
    a = push(mine, (2, 0))
    b = push(mine, (3, 0))
    c = push(mine, (1, 0))
    e = push(mine + c, (0, 3), (2, 1))
    d = push(jnp.concatenate([mine, b]), (0, 1), (2, 3))
    f = push(jnp.concatenate([e, again]), (3, 2))
    from_01 = part_01 + c + is_1 * d[:n] + is_3 * e + f[:n]
    from_23 = part_23 + a + b + is_1 * e + d[n:] + is_3 * d[:n] + f[n:]
    return from_01 + from_23


def per_device(
    grad_parts,
    gauss_noise,
    blt_buffers,
    blt_decays,
    blt_weights,
    master_weights,
    row_stat,
    col_stat,
):
    rows, cols = gauss_noise.shape
    n_col, n_run, n_plane = (lax.axis_size(axes) for axes in (COL, RUN, PLANE))
    arrived = lax.all_to_all(
        grad_parts.reshape(-1, rows, cols), "dp", split_axis=0, concat_axis=0, tiled=True
    )
    correlated = gauss_noise - jnp.sum(blt_buffers * blt_weights[:, None, None], axis=0)
    new_buffers = blt_decays[:, None, None] * blt_buffers + correlated[None]
    to = jnp.arange(n_run)
    same_cols = (to % 2 == lax.axis_index("core")).astype(jnp.float32)
    same_rows = (to // 2 == lax.axis_index("zl")).astype(jnp.float32)
    takes = jnp.concatenate(
        [
            jnp.broadcast_to(same_cols[:, None], (n_run, cols)),
            jnp.ones((n_run, rows), jnp.float32),
            jnp.broadcast_to(same_rows[:, None], (n_run, rows)),
        ],
        axis=1,
    )
    ones = jnp.broadcast_to(same_cols[0] + same_cols[1], (rows, rows))
    zh = lax.axis_index("zh")
    is_01, is_1, is_3 = (
        jnp.broadcast_to(here.astype(jnp.float32), (2 * rows,)) for here in (zh < 2, zh == 1, zh == 3)
    )
    arrived, correlated, new_buffers, takes, row_stat, ones, is_01, is_1, is_3 = lax.optimization_barrier(
        (arrived, correlated, new_buffers, takes, row_stat, ones, is_01, is_1, is_3)
    )
    noisy = arrived.sum(axis=0) + NOISE_STD * correlated
    squares = noisy * noisy
    share = DECAY_RATE / n_col * row_stat + (1.0 - DECAY_RATE) * (
        jnp.sum(squares, axis=1) / FF + TINY_TERM / n_col
    )
    sums = jnp.concatenate([jnp.sum(squares, axis=0), share, share])
    sums, col_stat, master_weights, takes = lax.optimization_barrier(
        (sums, col_stat, master_weights, takes)
    )
    run = sum_of_sent(sums[None] * takes, RUN)
    run, own = lax.optimization_barrier((run, run[cols + rows :]))
    plane = sum_of_sent(jnp.broadcast_to(run[None], (n_plane, *run.shape)), PLANE)
    stats = jnp.concatenate([plane[cols : cols + rows], own])
    new_col = DECAY_RATE * col_stat + (1.0 - DECAY_RATE) * (plane[:cols] / D + TINY_TERM)
    part_01, part_23 = is_01 * stats, (1.0 - is_01) * stats
    stats, new_col, part_01, part_23 = lax.optimization_barrier((stats, new_col, part_01, part_23))
    stats = sum_over_zh(stats, part_01, part_23, is_1, is_3)
    shares, new_row = lax.optimization_barrier((stats[:rows], stats[rows:]))
    row_mean = jnp.sum(ones * shares[None, :], axis=1) / D
    direction = noisy / jnp.sqrt((new_row / row_mean)[:, None] * new_col[None, :])
    weight_copy = (master_weights - LEARN_RATE * direction).astype(jnp.bfloat16)
    return (direction, weight_copy, new_buffers, new_row, new_col)


def solution(mesh):
    finer = Mesh(
        mesh.devices.reshape(mesh.shape["dp"], 4, 4, 4, 2),
        ("dp", "x", "zl", "zh", "core"),
    )
    rows = ("dp", *ROW)
    return jax.shard_map(
        per_device,
        mesh=finer,
        in_specs=(
            P("dp", None, ROW, COL),
            P(rows, COL),
            P(None, rows, COL),
            P(),
            P(),
            P(rows, COL),
            P(rows),
            P(COL),
        ),
        out_specs=(P(rows, COL), P(rows, COL), P(None, rows, COL), P(rows), P(COL)),
        check_vma=False,
    )
```
